128 devices in a mesh: member: 8 (over z, core), region: 16 (over y, x).
Axes of the slice: x: 4, y: 4, z: 4, core: 2. Of those that a mesh axis runs over, the one named last changes fastest.
Arguments:
- ensemble: bfloat16 [256, 1024, 512], P(('member', 'region')), may hold values from -6 to 6
- obs_site: int32 [1024, 2048], P(('member', 'region')), may hold values from 0 to 511
- obs_blocks: int32 [1024], P(('member', 'region')), may hold values from 1 to 16
- obs_precision: bfloat16 [1024, 2048], P(('member', 'region')), may hold values from 0.049804688 to 1
- obs_innovation: bfloat16 [1024, 2048], P(('member', 'region')), may hold values from -6 to 6
Outputs:
- analysis: bfloat16 [256, 1024, 512], P(('member', 'region'))
The draws below stay inside these ranges and needn't reach their ends.
Inputs may be any that keep to these rules, and one draw needn't show every extreme that they name: Only the first obs_blocks[p] blocks of 128 observations of patch p are used.
All inputs are finite; a program needn't handle non-finite values.
Results may differ from the reference program's by a relative error of at most 0.0062.
Values may be sent and summed in bfloat16 or wider, within the bound.
A program may use at most 64 MiB of HBM per device.

```python
import math
import jax
import jax.numpy as jnp
from jax import lax

K = 256
S = 512
OB = 128
BMAX = 16
ITERS = 6
P_SIZE = 1024


def with_ends(drawn, own_key, least, top_value):
    spot = [jax.random.randint(jax.random.fold_in(own_key, axis), (), 0, length) for axis, length in enumerate(drawn.shape)]
    main_axis = drawn.shape.index(max(drawn.shape))
    neighbour = spot[:main_axis] + [(spot[main_axis] + 1) % drawn.shape[main_axis]] + spot[main_axis + 1:]
    return drawn.at[tuple(spot)].set(least).at[tuple(neighbour)].set(top_value)


def steps_of(rng, dims, cuts, smallest, top_value):
    factor_of = 1.0
    for axis_at, parts in cuts:
        heights = jax.random.uniform(jax.random.fold_in(jax.random.fold_in(rng, 6), axis_at), (parts,), jnp.float32, smallest / len(cuts), top_value / len(cuts))
        factor_of = factor_of * jnp.repeat(jnp.exp(heights), dims[axis_at] // parts).reshape((-1,) + (1,) * (len(dims) - 1 - axis_at))
    return factor_of


def scatter_about(stream_key, extent, spread, bound, shards=(), held_as=jnp.bfloat16):
    level = steps_of(stream_key, extent, shards, -0.22, 0.18) if shards else 1.0
    values = jax.random.normal(stream_key, extent, jnp.float32) * spread * level
    return jnp.minimum(jnp.maximum(values, -bound), bound).astype(held_as)


def setup_inputs(seed: int = 0) -> dict:
    key_list = jax.random.split(jax.random.key(seed), 6)
    ensemble = scatter_about(key_list[0], (K, P_SIZE, S), 1.0, 6.0, ((0, 128),))
    obs_site = with_ends(jax.random.randint(key_list[1], (P_SIZE, BMAX * OB), 0, S), jax.random.fold_in(key_list[1], 1), 0, S - 1).astype(jnp.int32)
    obs_blocks = with_ends(jax.random.randint(key_list[2], (P_SIZE,), 1, BMAX + 1), jax.random.fold_in(key_list[2], 1), 1, BMAX).astype(jnp.int32)
    obs_precision = jnp.clip(jnp.exp(math.log(1.0) - 2.9996462 * jax.random.uniform(key_list[3], (P_SIZE, BMAX * OB), jnp.float32) ** steps_of(key_list[3], (P_SIZE, BMAX * OB), ((0, 128),), -0.2, 0.2)), 0.049804688, 1.0).astype(jnp.bfloat16)
    obs_innovation = scatter_about(key_list[4], (P_SIZE, BMAX * OB), 1.0, 6.0, ((0, 128),))
    return {"ensemble": ensemble, "obs_site": obs_site, "obs_blocks": obs_blocks, "obs_precision": obs_precision, "obs_innovation": obs_innovation}


def matmul_high(left, right):
    return jnp.matmul(left, right, precision=lax.Precision.HIGHEST)

def transform_weights(gram, rhs):
    members = gram.shape[-1]
    eye = jnp.eye(members, dtype=jnp.float32)
    amat = (members - 1.0) * eye + gram
    scale = jnp.sqrt(lax.optimization_barrier(jnp.sum(amat * amat, axis=(-2, -1))))[..., None, None]
    yk = amat / scale
    zk = jnp.broadcast_to(eye, amat.shape)
    for step in range(ITERS):
        tk = 1.5 * eye - 0.5 * matmul_high(zk, yk)
        yk = matmul_high(yk, tk)
        zk = matmul_high(tk, zk)
    wmean = matmul_high(zk, matmul_high(zk, rhs[..., None]))[..., 0] / scale[..., 0]
    coef = wmean[..., :, None] + jnp.sqrt(members - 1.0) * zk / jnp.sqrt(scale)
    return coef.astype(jnp.bfloat16)

def one_patch(items):
    member_rows, sites, blocks, precision, innovation = items
    values = member_rows.astype(jnp.float32)
    mean = lax.optimization_barrier(jnp.mean(values, axis=0))
    pert = (values - mean[None, :]).astype(jnp.bfloat16)
    slots = jnp.arange(sites.shape[0], dtype=jnp.int32) // OB
    live = jnp.where(slots < blocks, precision.astype(jnp.float32), jnp.float32(0.0))
    cols = jnp.take(pert, sites, axis=1)
    scaled = (cols.astype(jnp.float32) * live[None, :]).astype(jnp.bfloat16)
    gram = lax.dot_general(scaled, cols, (((1,), (1,)), ((), ())), preferred_element_type=jnp.float32)
    rhs = jnp.dot(scaled, innovation, preferred_element_type=jnp.float32)
    coef = transform_weights(gram, rhs)
    update = jnp.dot(coef.T, pert, preferred_element_type=jnp.float32)
    return (mean[None, :] + update).astype(jnp.bfloat16)

def reference(ensemble, obs_site, obs_blocks, obs_precision, obs_innovation):
    by_patch = jnp.transpose(ensemble, (1, 0, 2))
    result = lax.map(one_patch, (by_patch, obs_site, obs_blocks, obs_precision, obs_innovation))
    return jnp.transpose(result, (1, 0, 2))
```

```python
import functools

import jax
import jax.numpy as jnp
from jax import lax
from jax.experimental import pallas as pl
from jax.experimental.pallas import tpu as pltpu
from jax.sharding import PartitionSpec as P

K = 256
S = 512
SLOTS = 2048
OB = 128
ITERS = 6
DEVICES = 128
PATCHES = 8
GROUPS = 2
QUAD = PATCHES // GROUPS
STRIDE = 37
MESH = pl.DeviceIdType.MESH
F32 = jnp.float32
BF16 = jnp.bfloat16


def dot(left, right):
    return jnp.dot(left, right, preferred_element_type=F32)


def dot_t(left, right):
    return lax.dot_general(left, right, (((1,), (1,)), ((), ())), preferred_element_type=F32)


def split(value):
    high = value.astype(BF16)
    return high, (value - high.astype(F32)).astype(BF16)


def iota(shape, axis):
    return lax.broadcasted_iota(jnp.int32, shape, axis)


def peer(member, region, offset):
    x = lax.rem(lax.rem(region, 4) + lax.rem(offset, 4), 4)
    y = lax.rem(lax.div(region, 4) + lax.rem(lax.div(offset, 4), 4), 4)
    z = lax.rem(lax.div(member, 2) + lax.rem(lax.div(offset, 16), 4), 4)
    core = lax.rem(lax.rem(member, 2) + lax.div(offset, 64), 2)
    return z * 2 + core, y * 4 + x


def enter(member, region):
    barrier = pltpu.get_barrier_semaphore()
    members = [lax.rem(member + step, 8) for step in range(8)]
    regions = [lax.rem(region + step, 16) for step in range(16)]
    for outer in range(8):
        for inner in range(16):
            if outer or inner:
                pl.semaphore_signal(
                    barrier,
                    inc=1,
                    device_id=(members[outer], regions[inner]),
                    device_id_type=MESH,
                )
    pl.semaphore_wait(barrier, DEVICES - 1)


def histogram(site_ref, blocks_ref, weight32, value32, weights, sides):
    lanes = iota((1, SLOTS), 1)
    rows = iota((16, SLOTS), 0)
    quarter = lax.rem(rows, 4)

    def one(patch, carry):
        site = site_ref[pl.ds(patch, 1), :]
        live = lanes < blocks_ref[patch] * OB
        weight = jnp.where(live, weight32[pl.ds(patch, 1), :], 0.0)
        product = weight * value32[pl.ds(patch, 1), :]
        high = product.astype(BF16).astype(F32)
        low = product - high
        picked = jnp.where(rows < 4, weight, jnp.where(rows < 8, high, low))
        upper = jnp.where(quarter == lax.shift_right_logical(site, 7), picked, 0.0).astype(BF16)
        lower = jnp.where(iota((128, SLOTS), 0) == jnp.bitwise_and(site, 127), 1.0, 0.0).astype(BF16)
        sums = dot_t(upper, lower)
        weights[patch] = sums[0:4]
        sides[patch] = sums[4:8] + sums[8:12]
        return carry

    lax.fori_loop(0, PATCHES, one, 0)


def as_row(table):
    return jnp.concatenate([table[part : part + 1, :] for part in range(4)], axis=1)


def analyse(group, inbox, outbox, place_in, place_out, weights, sides, state, pert, work, zed, why, mean):
    landed = inbox.reshape(GROUPS, 4, 4 * K, 128)
    leaving = outbox.reshape(GROUPS, 4, 4 * K, 128)
    quads = range(QUAD)

    for block in range(4):
        rows = slice(256 * block, 256 * block + 256)
        for half in range(2):
            tile = jnp.concatenate([landed[group, 2 * half, rows, :], landed[group, 2 * half + 1, rows, :]], axis=1)
            placed = dot(place_in[...], tile).astype(BF16)
            for quad in quads:
                state[quad, 64 * block : 64 * block + 64, 256 * half : 256 * half + 256] = placed[
                    64 * quad : 64 * quad + 64
                ]

    eye = jnp.where(iota((K, K), 0) == iota((K, K), 1), 1.0, 0.0).astype(F32)
    scales, rights = [], []
    for quad in quads:
        values = state[quad].astype(F32)
        centre = jnp.sum(values, axis=0, keepdims=True) * (1.0 / K)
        mean[quad] = centre
        around = (values - centre).astype(BF16)
        pert[quad] = around
        work[quad, 0:K, :] = (around.astype(F32) * as_row(weights[group * QUAD + quad])).astype(BF16)
        side = as_row(sides[group * QUAD + quad])
        high = side.astype(BF16).astype(F32)
        work[quad, K : K + 16, :] = jnp.where(
            iota((16, S), 0) == 0, high, jnp.where(iota((16, S), 0) == 1, side - high, 0.0)
        ).astype(BF16)
    for quad in quads:
        sums = dot_t(work[quad], pert[quad])
        right = sums[K : K + 1] + sums[K + 1 : K + 2]
        amat = sums[0:K] + 255.0 * eye
        square = jnp.sum(jnp.sum(amat * amat, axis=0, keepdims=True), axis=1, keepdims=True)
        scale = jnp.sqrt(square)
        scales.append(scale)
        rights.append(right)
        why[quad] = amat / scale

    for quad in quads:
        first = why[quad]
        high = first.astype(BF16)
        zed[quad] = 1.5 * eye - 0.5 * first
        why[quad] = 1.5 * first - 0.5 * dot(high, high)
    for step in range(1, ITERS):
        exact = step >= ITERS - 2
        last = step == ITERS - 1
        for quad in quads:
            z, y = zed[quad], why[quad]
            if exact:
                z_high, z_low = split(z)
                y_high, y_low = split(y)
                w = dot(z_high, y_high) + dot(z_high, y_low) + dot(z_low, y_high)
                w_high, w_low = split(w)
                zed[quad] = 1.5 * z - 0.5 * (dot(z_high, w_high) + dot(z_high, w_low) + dot(z_low, w_high))
                if not last:
                    why[quad] = 1.5 * y - 0.5 * (dot(y_high, w_high) + dot(y_high, w_low) + dot(y_low, w_high))
            else:
                z_high, y_high = z.astype(BF16), y.astype(BF16)
                w_high = dot(z_high, y_high).astype(BF16)
                zed[quad] = 1.5 * z - 0.5 * dot(z_high, w_high)
                why[quad] = 1.5 * y - 0.5 * dot(y_high, w_high)

    for quad in quads:
        z = zed[quad]
        once = jnp.sum(z * rights[quad], axis=1, keepdims=True)
        twice = jnp.sum(z * once, axis=0, keepdims=True)
        factor = jnp.sqrt(255.0 / scales[quad])
        coef = (twice / scales[quad] + factor * z).astype(BF16)
        state[quad] = (mean[quad] + dot(coef, pert[quad])).astype(BF16)

    for block in range(4):
        rows = slice(256 * block, 256 * block + 256)
        for half in range(2):
            tile = jnp.concatenate(
                [state[quad, 64 * block : 64 * block + 64, 256 * half : 256 * half + 256] for quad in quads], axis=0
            )
            placed = dot(place_out[...], tile).astype(BF16)
            leaving[group, 2 * half, rows, :] = placed[:, 0:128]
            leaving[group, 2 * half + 1, rows, :] = placed[:, 128:256]


def kernel(
    ens_ref, site_ref, blocks_ref, precision_ref, innovation_ref, out_ref,
    inbox, outbox, place_in, place_out, weight32, value32, weights, sides, state, pert, work, zed, why, mean,
    in_send, in_recv, in_own, out_send, out_recv, out_own,
):
    member, region = lax.axis_index("member"), lax.axis_index("region")
    me = member * 16 + region

    enter(member, region)

    for group in range(GROUPS):
        pairs = pl.ds(2 * group, 2)

        def send(index, carry):
            to_member, to_region = peer(member, region, lax.rem(index * STRIDE, DEVICES))
            to = to_member * 16 + to_region
            for row in range(2):
                pltpu.make_async_remote_copy(
                    src_ref=ens_ref.at[row, to, :, pairs],
                    dst_ref=inbox.at[group, :, me, row],
                    send_sem=in_send.at[group],
                    recv_sem=in_recv.at[group],
                    device_id=(to_member, to_region),
                    device_id_type=MESH,
                ).start()
            return carry

        lax.fori_loop(1, DEVICES, send, 0)
        for row in range(2):
            pltpu.make_async_copy(
                ens_ref.at[row, me, :, pairs], inbox.at[group, :, me, row], in_own.at[group, row]
            ).start()

    out_row, in_row = iota((256, 256), 0), iota((256, 256), 1)
    moved = jnp.bitwise_and(out_row, 63) * 4 + lax.shift_right_logical(out_row, 6)
    place_in[...] = jnp.where(in_row == moved, 1.0, 0.0).astype(BF16)
    moved = jnp.bitwise_and(out_row, 3) * 64 + lax.shift_right_logical(out_row, 2)
    place_out[...] = jnp.where(in_row == moved, 1.0, 0.0).astype(BF16)
    weight32[...] = precision_ref[...].astype(F32)
    value32[...] = innovation_ref[...].astype(F32)
    histogram(site_ref, blocks_ref, weight32, value32, weights, sides)

    def one_group(group, carry):
        pairs = pl.ds(2 * group, 2)
        for row in range(2):
            pltpu.make_async_copy(
                ens_ref.at[row, me, :, pairs], inbox.at[group, :, me, row], in_own.at[group, row]
            ).wait()
        arrived = inbox.at[group, :, pl.ds(0, DEVICES - 1)]
        pltpu.make_async_copy(arrived, arrived, in_recv.at[group]).wait()

        analyse(
            group, inbox, outbox, place_in, place_out, weights, sides, state, pert, work, zed, why, mean
        )

        def send(index, carry):
            to_member, to_region = peer(member, region, lax.rem(index * STRIDE, DEVICES))
            to = to_member * 16 + to_region
            for row in range(2):
                pltpu.make_async_remote_copy(
                    src_ref=outbox.at[group, :, to, row],
                    dst_ref=out_ref.at[row, me, :, pairs],
                    send_sem=out_send,
                    recv_sem=out_recv,
                    device_id=(to_member, to_region),
                    device_id_type=MESH,
                ).start()
            return carry

        lax.fori_loop(1, DEVICES, send, 0)
        for row in range(2):
            pltpu.make_async_copy(
                outbox.at[group, :, me, row], out_ref.at[row, me, :, pairs], out_own.at[group, row]
            ).start()
        return carry

    lax.fori_loop(0, GROUPS, one_group, 0)

    for group in range(GROUPS):
        sent = inbox.at[group, :, pl.ds(0, DEVICES - 1)]
        pltpu.make_async_copy(sent, sent, in_send.at[group]).wait()
        for row in range(2):
            pltpu.make_async_copy(
                outbox.at[group, :, me, row], out_ref.at[row, me, :, pl.ds(2 * group, 2)], out_own.at[group, row]
            ).wait()
    sent = outbox.at[:, :, pl.ds(0, DEVICES - 1)]
    pltpu.make_async_copy(sent, sent, out_send).wait()
    arrived = out_ref.at[:, pl.ds(0, DEVICES - 1)]
    pltpu.make_async_copy(arrived, arrived, out_recv).wait()


def local(ensemble, obs_site, obs_blocks, obs_precision, obs_innovation):
    pairs = ensemble.reshape(2, DEVICES, PATCHES, 4, 128).transpose(0, 1, 3, 2, 4)
    pairs = pairs.reshape(2, DEVICES, 4, 4, 2, 128)
    vmem = pl.BlockSpec(memory_space=pltpu.VMEM)
    hbm = pl.BlockSpec(memory_space=pltpu.HBM)
    result = pl.pallas_call(
        kernel,
        out_shape=jax.ShapeDtypeStruct(pairs.shape, BF16),
        in_specs=[hbm, vmem, pl.BlockSpec(memory_space=pltpu.SMEM), vmem, vmem],
        out_specs=hbm,
        scratch_shapes=[
            pltpu.VMEM((GROUPS, 4, DEVICES, 2, 2, 2, 128), BF16),
            pltpu.VMEM((GROUPS, 4, DEVICES, 2, 2, 2, 128), BF16),
            pltpu.VMEM((256, 256), BF16),
            pltpu.VMEM((256, 256), BF16),
            pltpu.VMEM((PATCHES, SLOTS), F32),
            pltpu.VMEM((PATCHES, SLOTS), F32),
            pltpu.VMEM((PATCHES, 4, 128), F32),
            pltpu.VMEM((PATCHES, 4, 128), F32),
            pltpu.VMEM((QUAD, K, S), BF16),
            pltpu.VMEM((QUAD, K, S), BF16),
            pltpu.VMEM((QUAD, K + 16, S), BF16),
            pltpu.VMEM((QUAD, K, K), F32),
            pltpu.VMEM((QUAD, K, K), F32),
            pltpu.VMEM((QUAD, 1, S), F32),
            pltpu.SemaphoreType.DMA((GROUPS,)),
            pltpu.SemaphoreType.DMA((GROUPS,)),
            pltpu.SemaphoreType.DMA((GROUPS, 2)),
            pltpu.SemaphoreType.DMA,
            pltpu.SemaphoreType.DMA,
            pltpu.SemaphoreType.DMA((GROUPS, 2)),
        ],
        compiler_params=pltpu.CompilerParams(
            collective_id=0, has_side_effects=True, vmem_limit_bytes=56 * 1024 * 1024
        ),
    )(pairs, obs_site, obs_blocks, obs_precision, obs_innovation)
    result = result.reshape(2, DEVICES, 4, PATCHES, 128).transpose(0, 1, 3, 2, 4)
    return result.reshape(2, DEVICES * PATCHES, S)


def solution(mesh):
    axes = ("member", "region")
    rows = P(axes, None)
    return jax.shard_map(
        local,
        mesh=mesh,
        in_specs=(P(axes, None, None), rows, P(axes), rows, rows),
        out_specs=P(axes, None, None),
        check_vma=False,
    )
```

```python
import functools

import jax
import jax.numpy as jnp
from jax import lax
from jax.experimental import pallas as pl
from jax.experimental.pallas import tpu as pltpu
from jax.sharding import PartitionSpec as P

K = 256
S = 512
SLOTS = 2048
OB = 128
ITERS = 6
EXACT_FROM = 4
DEVICES = 128
PATCHES = 8
GROUPS = 2
QUAD = PATCHES // GROUPS
STRIDE = 37
MESH = pl.DeviceIdType.MESH
F32 = jnp.float32
BF16 = jnp.bfloat16


def dot(left, right):
    return jnp.dot(left, right, preferred_element_type=F32)


def dot_t(left, right):
    return lax.dot_general(left, right, (((1,), (1,)), ((), ())), preferred_element_type=F32)


def split(value):
    high = value.astype(BF16)
    return high, (value - high.astype(F32)).astype(BF16)


def iota(shape, axis):
    return lax.broadcasted_iota(jnp.int32, shape, axis)


def peer(member, region, offset):
    x = lax.rem(lax.rem(region, 4) + lax.rem(offset, 4), 4)
    y = lax.rem(lax.div(region, 4) + lax.rem(lax.div(offset, 4), 4), 4)
    z = lax.rem(lax.div(member, 2) + lax.rem(lax.div(offset, 16), 4), 4)
    core = lax.rem(lax.rem(member, 2) + lax.div(offset, 64), 2)
    return z * 2 + core, y * 4 + x


def enter(member, region):
    barrier = pltpu.get_barrier_semaphore()
    members = [lax.rem(member + step, 8) for step in range(8)]
    regions = [lax.rem(region + step, 16) for step in range(16)]
    for outer in range(8):
        for inner in range(16):
            if outer or inner:
                pl.semaphore_signal(
                    barrier,
                    inc=1,
                    device_id=(members[outer], regions[inner]),
                    device_id_type=MESH,
                )
    pl.semaphore_wait(barrier, DEVICES - 1)


def histogram(site_ref, blocks_ref, weight32, value32, weights, sides):
    lanes = iota((1, SLOTS), 1)
    rows = iota((16, SLOTS), 0)
    quarter = lax.rem(rows, 4)

    def one(patch, carry):
        site = site_ref[pl.ds(patch, 1), :]
        live = lanes < blocks_ref[patch] * OB
        weight = jnp.where(live, weight32[pl.ds(patch, 1), :], 0.0)
        product = weight * value32[pl.ds(patch, 1), :]
        high = product.astype(BF16).astype(F32)
        low = product - high
        picked = jnp.where(rows < 4, weight, jnp.where(rows < 8, high, low))
        upper = jnp.where(quarter == lax.shift_right_logical(site, 7), picked, 0.0).astype(BF16)
        lower = jnp.where(iota((128, SLOTS), 0) == jnp.bitwise_and(site, 127), 1.0, 0.0).astype(BF16)
        sums = dot_t(upper, lower)
        weights[patch] = sums[0:4]
        sides[patch] = sums[4:8] + sums[8:12]
        return carry

    lax.fori_loop(0, PATCHES, one, 0)


def as_row(table):
    return jnp.concatenate([table[part : part + 1, :] for part in range(4)], axis=1)


def analyse(group, inbox, outbox, place_in, place_out, weights, sides, state, pert, work, iterate, high_part, low_part, product, product_low, coef, mean):
    landed = inbox.reshape(GROUPS, 4, 4 * K, 128)
    leaving = outbox.reshape(GROUPS, 4, 4 * K, 128)
    quads = range(QUAD)

    for block in range(4):
        rows = slice(256 * block, 256 * block + 256)
        for half in range(2):
            tile = jnp.concatenate([landed[group, 2 * half, rows, :], landed[group, 2 * half + 1, rows, :]], axis=1)
            placed = dot(place_in[...], tile).astype(BF16)
            for quad in quads:
                state[quad, 64 * block : 64 * block + 64, 256 * half : 256 * half + 256] = placed[
                    64 * quad : 64 * quad + 64
                ]

    eye = jnp.where(iota((K, K), 0) == iota((K, K), 1), 1.0, 0.0).astype(F32)
    scales, rights = [], []
    for quad in quads:
        values = state[quad].astype(F32)
        centre = jnp.sum(values, axis=0, keepdims=True) * (1.0 / K)
        mean[quad] = centre
        around = (values - centre).astype(BF16)
        pert[quad] = around
        work[quad, 0:K, :] = (around.astype(F32) * as_row(weights[group * QUAD + quad])).astype(BF16)
        side = as_row(sides[group * QUAD + quad])
        high = side.astype(BF16).astype(F32)
        work[quad, K : K + 16, :] = jnp.where(
            iota((16, S), 0) == 0, high, jnp.where(iota((16, S), 0) == 1, side - high, 0.0)
        ).astype(BF16)
    for quad in quads:
        sums = dot_t(work[quad], pert[quad])
        right = sums[K : K + 1] + sums[K + 1 : K + 2]
        amat = sums[0:K] + 255.0 * eye
        square = jnp.sum(jnp.sum(amat * amat, axis=0, keepdims=True), axis=1, keepdims=True)
        scale = jnp.sqrt(square)
        scales.append(scale)
        rights.append(right)
        first = amat / scale
        iterate[quad, K:] = first
        high_part[quad, K:] = first.astype(BF16)
    for quad in quads:
        first = iterate[quad, K:]
        second = (eye - first * (1.0 / 3.0), first - dot(high_part[quad, K:], high_part[quad, K:]) * (1.0 / 3.0))
        for part in range(2):
            iterate[quad, K * part : K * part + K] = second[part]
            high_part[quad, K * part : K * part + K] = second[part].astype(BF16)

    for step in range(1, ITERS):
        exact = step >= EXACT_FROM
        last = step == ITERS - 1
        third = 1.5 ** (2 * step) / 3.0
        for quad in quads:
            z_high, y_high = high_part[quad, 0:K], high_part[quad, K:]
            both = dot(z_high, y_high)
            if exact:
                both += dot(z_high, low_part[quad, K:]) + dot(low_part[quad, 0:K], y_high)
                both = both * third
                product_low[quad] = (both - both.astype(BF16).astype(F32)).astype(BF16)
                product[quad] = both.astype(BF16)
            else:
                product[quad] = (both * third).astype(BF16)
        for quad in quads:
            for part in range(1 if last else 2):
                rows = slice(K * part, K * part + K)
                high = high_part[quad, rows]
                moved = dot(high, product[quad])
                if exact:
                    moved += dot(high, product_low[quad]) + dot(low_part[quad, rows], product[quad])
                after = iterate[quad, rows] - moved
                iterate[quad, rows] = after
                if not last:
                    high_part[quad, rows] = after.astype(BF16)
                    if step + 1 >= EXACT_FROM:
                        low_part[quad, rows] = (after - after.astype(BF16).astype(F32)).astype(BF16)

    grown = 1.5**ITERS
    for quad in quads:
        z = iterate[quad, 0:K]
        once = jnp.sum(z * rights[quad], axis=1, keepdims=True)
        twice = jnp.sum(z * once, axis=0, keepdims=True)
        factor = grown * jnp.sqrt(255.0 / scales[quad])
        coef[quad] = (twice * (grown * grown / scales[quad]) + factor * z).astype(BF16)
    for quad in quads:
        state[quad] = (mean[quad] + dot(coef[quad], pert[quad])).astype(BF16)

    for block in range(4):
        rows = slice(256 * block, 256 * block + 256)
        for half in range(2):
            tile = jnp.concatenate(
                [state[quad, 64 * block : 64 * block + 64, 256 * half : 256 * half + 256] for quad in quads], axis=0
            )
            placed = dot(place_out[...], tile).astype(BF16)
            leaving[group, 2 * half, rows, :] = placed[:, 0:128]
            leaving[group, 2 * half + 1, rows, :] = placed[:, 128:256]


def kernel(
    ens_ref, site_hbm, blocks_hbm, precision_hbm, innovation_hbm, out_ref,
    site_ref, blocks_ref, precision_ref, innovation_ref, inbox, outbox, place_in, place_out, weight32, value32, weights, sides, state, pert, work, iterate, high_part, low_part, product, product_low, coef, mean,
    obs_sem, in_send, in_recv, in_own, out_send, out_recv, out_own,
):
    member, region = lax.axis_index("member"), lax.axis_index("region")
    me = member * 16 + region

    moves = (
        pltpu.make_async_copy(site_hbm, site_ref, obs_sem.at[0]),
        pltpu.make_async_copy(precision_hbm, precision_ref, obs_sem.at[1]),
        pltpu.make_async_copy(innovation_hbm, innovation_ref, obs_sem.at[2]),
        pltpu.make_async_copy(blocks_hbm, blocks_ref, obs_sem.at[3]),
    )
    for move in moves:
        move.start()
    enter(member, region)

    for group in range(GROUPS):
        def send(index, carry):
            to_member, to_region = peer(member, region, lax.rem(index * STRIDE, DEVICES))
            to = to_member * 16 + to_region
            for row in range(2):
                pltpu.make_async_remote_copy(
                    src_ref=ens_ref.at[row, to, :, group],
                    dst_ref=inbox.at[group, :, me, row],
                    send_sem=in_send.at[group],
                    recv_sem=in_recv.at[group],
                    device_id=(to_member, to_region),
                    device_id_type=MESH,
                ).start()
            return carry

        lax.fori_loop(1, DEVICES, send, 0)
        for row in range(2):
            pltpu.make_async_copy(
                ens_ref.at[row, me, :, group], inbox.at[group, :, me, row], in_own.at[group, row]
            ).start()

    out_row, in_row = iota((256, 256), 0), iota((256, 256), 1)
    moved = jnp.bitwise_and(out_row, 63) * 4 + lax.shift_right_logical(out_row, 6)
    place_in[...] = jnp.where(in_row == moved, 1.0, 0.0).astype(BF16)
    moved = jnp.bitwise_and(out_row, 3) * 64 + lax.shift_right_logical(out_row, 2)
    place_out[...] = jnp.where(in_row == moved, 1.0, 0.0).astype(BF16)
    for move in moves:
        move.wait()
    weight32[...] = precision_ref[...].astype(F32)
    value32[...] = innovation_ref[...].astype(F32)
    histogram(site_ref, blocks_ref, weight32, value32, weights, sides)

    def one_group(group, carry):
        for row in range(2):
            pltpu.make_async_copy(
                ens_ref.at[row, me, :, group], inbox.at[group, :, me, row], in_own.at[group, row]
            ).wait()
        arrived = inbox.at[group, :, pl.ds(0, DEVICES - 1)]
        pltpu.make_async_copy(arrived, arrived, in_recv.at[group]).wait()

        analyse(
            group, inbox, outbox, place_in, place_out, weights, sides, state, pert, work, iterate, high_part, low_part, product, product_low, coef, mean
        )

        def send(index, carry):
            to_member, to_region = peer(member, region, lax.rem(index * STRIDE, DEVICES))
            to = to_member * 16 + to_region
            for row in range(2):
                pltpu.make_async_remote_copy(
                    src_ref=outbox.at[group, :, to, row],
                    dst_ref=out_ref.at[row, me, :, group],
                    send_sem=out_send,
                    recv_sem=out_recv,
                    device_id=(to_member, to_region),
                    device_id_type=MESH,
                ).start()
            return carry

        lax.fori_loop(1, DEVICES, send, 0)
        for row in range(2):
            pltpu.make_async_copy(
                outbox.at[group, :, me, row], out_ref.at[row, me, :, group], out_own.at[group, row]
            ).start()
        return carry

    lax.fori_loop(0, GROUPS, one_group, 0)

    for group in range(GROUPS):
        sent = inbox.at[group, :, pl.ds(0, DEVICES - 1)]
        pltpu.make_async_copy(sent, sent, in_send.at[group]).wait()
        for row in range(2):
            pltpu.make_async_copy(
                outbox.at[group, :, me, row], out_ref.at[row, me, :, group], out_own.at[group, row]
            ).wait()
    sent = outbox.at[:, :, pl.ds(0, DEVICES - 1)]
    pltpu.make_async_copy(sent, sent, out_send).wait()
    arrived = out_ref.at[:, pl.ds(0, DEVICES - 1)]
    pltpu.make_async_copy(arrived, arrived, out_recv).wait()


def local(ensemble, obs_site, obs_blocks, obs_precision, obs_innovation):
    pairs = ensemble.reshape(2, DEVICES, PATCHES, 4, 128).transpose(0, 1, 3, 2, 4)
    pairs = pairs.reshape(2, DEVICES, 4, GROUPS, QUAD, 128)
    hbm = pl.BlockSpec(memory_space=pltpu.HBM)
    result = pl.pallas_call(
        kernel,
        out_shape=jax.ShapeDtypeStruct(pairs.shape, BF16),
        in_specs=[hbm] * 5,
        out_specs=pl.BlockSpec(memory_space=pl.ANY),
        scratch_shapes=[
            pltpu.VMEM((PATCHES, SLOTS), jnp.int32),
            pltpu.SMEM((PATCHES,), jnp.int32),
            pltpu.VMEM((PATCHES, SLOTS), BF16),
            pltpu.VMEM((PATCHES, SLOTS), BF16),
            pltpu.VMEM((GROUPS, 4, DEVICES, 2, QUAD, 128), BF16),
            pltpu.VMEM((GROUPS, 4, DEVICES, 2, QUAD, 128), BF16),
            pltpu.VMEM((256, 256), BF16),
            pltpu.VMEM((256, 256), BF16),
            pltpu.VMEM((PATCHES, SLOTS), F32),
            pltpu.VMEM((PATCHES, SLOTS), F32),
            pltpu.VMEM((PATCHES, 4, 128), F32),
            pltpu.VMEM((PATCHES, 4, 128), F32),
            pltpu.VMEM((QUAD, K, S), BF16),
            pltpu.VMEM((QUAD, K, S), BF16),
            pltpu.VMEM((QUAD, K + 16, S), BF16),
            pltpu.VMEM((QUAD, 2 * K, K), F32),
            pltpu.VMEM((QUAD, 2 * K, K), BF16),
            pltpu.VMEM((QUAD, 2 * K, K), BF16),
            pltpu.VMEM((QUAD, K, K), BF16),
            pltpu.VMEM((QUAD, K, K), BF16),
            pltpu.VMEM((QUAD, K, K), BF16),
            pltpu.VMEM((QUAD, 1, S), F32),
            pltpu.SemaphoreType.DMA((4,)),
            pltpu.SemaphoreType.DMA((GROUPS,)),
            pltpu.SemaphoreType.DMA((GROUPS,)),
            pltpu.SemaphoreType.DMA((GROUPS, 2)),
            pltpu.SemaphoreType.DMA,
            pltpu.SemaphoreType.DMA,
            pltpu.SemaphoreType.DMA((GROUPS, 2)),
        ],
        compiler_params=pltpu.CompilerParams(
            collective_id=0, has_side_effects=True, vmem_limit_bytes=24 * 1024 * 1024
        ),
    )(*[pltpu.with_memory_space_constraint(arg, pltpu.HBM) for arg in (pairs, obs_site, obs_blocks, obs_precision, obs_innovation)])
    result = result.reshape(2, DEVICES, 4, PATCHES, 128).transpose(0, 1, 3, 2, 4)
    return result.reshape(2, DEVICES * PATCHES, S)


def solution(mesh):
    axes = ("member", "region")
    rows = P(axes, None)
    return jax.shard_map(
        local,
        mesh=mesh,
        in_specs=(P(axes, None, None), rows, P(axes), rows, rows),
        out_specs=P(axes, None, None),
        check_vma=False,
    )
```

```python
import functools

import jax
import jax.numpy as jnp
from jax import lax
from jax.experimental import pallas as pl
from jax.experimental.pallas import tpu as pltpu
from jax.sharding import PartitionSpec as P

K = 256
S = 512
SLOTS = 2048
OB = 128
ITERS = 6
EXACT_FROM = 4
DEVICES = 128
PATCHES = 8
GROUPS = 2
QUAD = PATCHES // GROUPS
STRIDE = 37
MESH = pl.DeviceIdType.MESH
F32 = jnp.float32
BF16 = jnp.bfloat16


def dot(left, right):
    return jnp.dot(left, right, preferred_element_type=F32)


def dot_t(left, right):
    return lax.dot_general(left, right, (((1,), (1,)), ((), ())), preferred_element_type=F32)


def split(value):
    high = value.astype(BF16)
    return high, (value - high.astype(F32)).astype(BF16)


def iota(shape, axis):
    return lax.broadcasted_iota(jnp.int32, shape, axis)


def hops(offset):
    return sum(min(step, 4 - step) for step in (offset % 4, offset // 4 % 4, offset // 16 % 4))


def spread(offset):
    return offset * STRIDE % DEVICES


OTHERS = sorted(range(1, DEVICES), key=spread)
FARTHEST_FIRST = sorted(OTHERS, key=lambda offset: (-hops(offset), spread(offset)))


def neighbours(member, region):
    xs = [lax.rem(lax.rem(region, 4) + step, 4) for step in range(4)]
    ys = [lax.rem(lax.div(region, 4) + step, 4) * 4 for step in range(4)]
    zs = [lax.rem(lax.div(member, 2) + step, 4) * 2 for step in range(4)]
    cores = [lax.rem(lax.rem(member, 2) + step, 2) for step in range(2)]

    def at(offset):
        return zs[offset // 16 % 4] + cores[offset // 64], ys[offset // 4 % 4] + xs[offset % 4]

    return at


def histogram(site_ref, blocks_ref, weight32, value32, weights, sides):
    lanes = iota((1, SLOTS), 1)
    rows = iota((16, SLOTS), 0)
    quarter = lax.rem(rows, 4)

    def one(patch, carry):
        site = site_ref[pl.ds(patch, 1), :]
        live = lanes < blocks_ref[patch] * OB
        weight = jnp.where(live, weight32[pl.ds(patch, 1), :], 0.0)
        product = weight * value32[pl.ds(patch, 1), :]
        high = product.astype(BF16).astype(F32)
        low = product - high
        picked = jnp.where(rows < 4, weight, jnp.where(rows < 8, high, low))
        upper = jnp.where(quarter == lax.shift_right_logical(site, 7), picked, 0.0).astype(BF16)
        lower = jnp.where(iota((128, SLOTS), 0) == jnp.bitwise_and(site, 127), 1.0, 0.0).astype(BF16)
        sums = dot_t(upper, lower)
        weights[patch] = sums[0:4]
        sides[patch] = sums[4:8] + sums[8:12]
        return carry

    lax.fori_loop(0, PATCHES, one, 0)


def as_row(table):
    return jnp.concatenate([table[part : part + 1, :] for part in range(4)], axis=1)


def analyse(group, inbox, outbox, place_in, place_out, weights, sides, state, pert, work, iterate, high_part, low_part, product, product_low, coef, mean):
    landed = inbox.reshape(GROUPS, 4, 4 * K, 128)
    leaving = outbox.reshape(GROUPS, 4, 4 * K, 128)
    quads = range(QUAD)

    for block in range(4):
        rows = slice(256 * block, 256 * block + 256)
        for half in range(2):
            tile = jnp.concatenate([landed[group, 2 * half, rows, :], landed[group, 2 * half + 1, rows, :]], axis=1)
            placed = dot(place_in[...], tile).astype(BF16)
            for quad in quads:
                state[quad, 64 * block : 64 * block + 64, 256 * half : 256 * half + 256] = placed[
                    64 * quad : 64 * quad + 64
                ]

    eye = jnp.where(iota((K, K), 0) == iota((K, K), 1), 1.0, 0.0).astype(F32)
    scales, rights = [], []
    for quad in quads:
        values = state[quad].astype(F32)
        centre = jnp.sum(values, axis=0, keepdims=True) * (1.0 / K)
        mean[quad] = centre
        around = (values - centre).astype(BF16)
        pert[quad] = around
        work[quad, 0:K, :] = (around.astype(F32) * as_row(weights[group * QUAD + quad])).astype(BF16)
        side = as_row(sides[group * QUAD + quad])
        high = side.astype(BF16).astype(F32)
        work[quad, K : K + 16, :] = jnp.where(
            iota((16, S), 0) == 0, high, jnp.where(iota((16, S), 0) == 1, side - high, 0.0)
        ).astype(BF16)
    for quad in quads:
        sums = dot_t(work[quad], pert[quad])
        right = sums[K : K + 1] + sums[K + 1 : K + 2]
        amat = sums[0:K] + 255.0 * eye
        square = jnp.sum(jnp.sum(amat * amat, axis=0, keepdims=True), axis=1, keepdims=True)
        scale = jnp.sqrt(square)
        scales.append(scale)
        rights.append(right)
        first = amat / scale
        iterate[quad, K:] = first
        high_part[quad, K:] = first.astype(BF16)
    for quad in quads:
        first = iterate[quad, K:]
        second = (eye - first * (1.0 / 3.0), first - dot(high_part[quad, K:], high_part[quad, K:]) * (1.0 / 3.0))
        for part in range(2):
            iterate[quad, K * part : K * part + K] = second[part]
            high_part[quad, K * part : K * part + K] = second[part].astype(BF16)

    for step in range(1, ITERS):
        exact = step >= EXACT_FROM
        last = step == ITERS - 1
        third = 1.5 ** (2 * step) / 3.0
        for quad in quads:
            z_high, y_high = high_part[quad, 0:K], high_part[quad, K:]
            both = dot(z_high, y_high)
            if exact:
                both += dot(z_high, low_part[quad, K:]) + dot(low_part[quad, 0:K], y_high)
                both = both * third
                product_low[quad] = (both - both.astype(BF16).astype(F32)).astype(BF16)
                product[quad] = both.astype(BF16)
            else:
                product[quad] = (both * third).astype(BF16)
        for quad in quads:
            for part in range(1 if last else 2):
                rows = slice(K * part, K * part + K)
                high = high_part[quad, rows]
                moved = dot(high, product[quad])
                if exact:
                    moved += dot(high, product_low[quad]) + dot(low_part[quad, rows], product[quad])
                after = iterate[quad, rows] - moved
                iterate[quad, rows] = after
                if not last:
                    high_part[quad, rows] = after.astype(BF16)
                    if step + 1 >= EXACT_FROM:
                        low_part[quad, rows] = (after - after.astype(BF16).astype(F32)).astype(BF16)

    grown = 1.5**ITERS
    for quad in quads:
        z = iterate[quad, 0:K]
        once = jnp.sum(z * rights[quad], axis=1, keepdims=True)
        twice = jnp.sum(z * once, axis=0, keepdims=True)
        factor = grown * jnp.sqrt(255.0 / scales[quad])
        coef[quad] = (twice * (grown * grown / scales[quad]) + factor * z).astype(BF16)
    for quad in quads:
        state[quad] = (mean[quad] + dot(coef[quad], pert[quad])).astype(BF16)

    for block in range(4):
        rows = slice(256 * block, 256 * block + 256)
        for half in range(2):
            tile = jnp.concatenate(
                [state[quad, 64 * block : 64 * block + 64, 256 * half : 256 * half + 256] for quad in quads], axis=0
            )
            placed = dot(place_out[...], tile).astype(BF16)
            leaving[group, 2 * half, rows, :] = placed[:, 0:128]
            leaving[group, 2 * half + 1, rows, :] = placed[:, 128:256]


def kernel(
    ens_ref, site_hbm, blocks_hbm, precision_hbm, innovation_hbm, out_ref,
    site_ref, blocks_ref, precision_ref, innovation_ref, inbox, outbox, place_in, place_out, weight32, value32, weights, sides, state, pert, work, iterate, high_part, low_part, product, product_low, coef, mean,
    obs_sem, in_send, in_recv, in_own, out_send, out_recv, out_own,
):
    member, region = lax.axis_index("member"), lax.axis_index("region")
    me = member * 16 + region

    moves = (
        pltpu.make_async_copy(site_hbm, site_ref, obs_sem.at[0]),
        pltpu.make_async_copy(precision_hbm, precision_ref, obs_sem.at[1]),
        pltpu.make_async_copy(innovation_hbm, innovation_ref, obs_sem.at[2]),
        pltpu.make_async_copy(blocks_hbm, blocks_ref, obs_sem.at[3]),
    )
    for move in moves:
        move.start()
    at = neighbours(member, region)

    def send_in(group, offsets):
        for offset in offsets:
            device = at(offset)
            for row in range(2):
                pltpu.make_async_remote_copy(
                    src_ref=ens_ref.at[row, device[0] * 16 + device[1], :, group],
                    dst_ref=inbox.at[group, :, me, row],
                    send_sem=in_send.at[group],
                    recv_sem=in_recv.at[group],
                    device_id=device,
                    device_id_type=MESH,
                ).start()

    barrier = pltpu.get_barrier_semaphore()
    for offset in FARTHEST_FIRST:
        pl.semaphore_signal(barrier, inc=1, device_id=at(offset), device_id_type=MESH)
    pl.semaphore_wait(barrier, DEVICES - 1)
    send_in(0, OTHERS)
    send_in(1, OTHERS)
    for group in range(GROUPS):
        for row in range(2):
            pltpu.make_async_copy(
                ens_ref.at[row, me, :, group], inbox.at[group, :, me, row], in_own.at[group, row]
            ).start()

    out_row, in_row = iota((256, 256), 0), iota((256, 256), 1)
    moved = jnp.bitwise_and(out_row, 63) * 4 + lax.shift_right_logical(out_row, 6)
    place_in[...] = jnp.where(in_row == moved, 1.0, 0.0).astype(BF16)
    moved = jnp.bitwise_and(out_row, 3) * 64 + lax.shift_right_logical(out_row, 2)
    place_out[...] = jnp.where(in_row == moved, 1.0, 0.0).astype(BF16)
    for move in moves:
        move.wait()
    weight32[...] = precision_ref[...].astype(F32)
    value32[...] = innovation_ref[...].astype(F32)
    histogram(site_ref, blocks_ref, weight32, value32, weights, sides)

    def one_group(group, carry):
        for row in range(2):
            pltpu.make_async_copy(
                ens_ref.at[row, me, :, group], inbox.at[group, :, me, row], in_own.at[group, row]
            ).wait()
        arrived = inbox.at[group, :, pl.ds(0, DEVICES - 1)]
        pltpu.make_async_copy(arrived, arrived, in_recv.at[group]).wait()

        analyse(
            group, inbox, outbox, place_in, place_out, weights, sides, state, pert, work, iterate, high_part, low_part, product, product_low, coef, mean
        )

        for offset in FARTHEST_FIRST:
            device = at(offset)
            for row in range(2):
                pltpu.make_async_remote_copy(
                    src_ref=outbox.at[group, :, device[0] * 16 + device[1], row],
                    dst_ref=out_ref.at[row, me, :, group],
                    send_sem=out_send,
                    recv_sem=out_recv,
                    device_id=device,
                    device_id_type=MESH,
                ).start()
        for row in range(2):
            pltpu.make_async_copy(
                outbox.at[group, :, me, row], out_ref.at[row, me, :, group], out_own.at[group, row]
            ).start()
        return carry

    lax.fori_loop(0, GROUPS, one_group, 0)

    for group in range(GROUPS):
        sent = inbox.at[group, :, pl.ds(0, DEVICES - 1)]
        pltpu.make_async_copy(sent, sent, in_send.at[group]).wait()
        for row in range(2):
            pltpu.make_async_copy(
                outbox.at[group, :, me, row], out_ref.at[row, me, :, group], out_own.at[group, row]
            ).wait()
    sent = outbox.at[:, :, pl.ds(0, DEVICES - 1)]
    pltpu.make_async_copy(sent, sent, out_send).wait()
    arrived = out_ref.at[:, pl.ds(0, DEVICES - 1)]
    pltpu.make_async_copy(arrived, arrived, out_recv).wait()


def local(ensemble, obs_site, obs_blocks, obs_precision, obs_innovation):
    pairs = ensemble.reshape(2, DEVICES, PATCHES, 4, 128).transpose(0, 1, 3, 2, 4)
    pairs = pairs.reshape(2, DEVICES, 4, GROUPS, QUAD, 128)
    hbm = pl.BlockSpec(memory_space=pltpu.HBM)
    result = pl.pallas_call(
        kernel,
        out_shape=jax.ShapeDtypeStruct(pairs.shape, BF16),
        in_specs=[hbm] * 5,
        out_specs=pl.BlockSpec(memory_space=pl.ANY),
        scratch_shapes=[
            pltpu.VMEM((PATCHES, SLOTS), jnp.int32),
            pltpu.SMEM((PATCHES,), jnp.int32),
            pltpu.VMEM((PATCHES, SLOTS), BF16),
            pltpu.VMEM((PATCHES, SLOTS), BF16),
            pltpu.VMEM((GROUPS, 4, DEVICES, 2, QUAD, 128), BF16),
            pltpu.VMEM((GROUPS, 4, DEVICES, 2, QUAD, 128), BF16),
            pltpu.VMEM((256, 256), BF16),
            pltpu.VMEM((256, 256), BF16),
            pltpu.VMEM((PATCHES, SLOTS), F32),
            pltpu.VMEM((PATCHES, SLOTS), F32),
            pltpu.VMEM((PATCHES, 4, 128), F32),
            pltpu.VMEM((PATCHES, 4, 128), F32),
            pltpu.VMEM((QUAD, K, S), BF16),
            pltpu.VMEM((QUAD, K, S), BF16),
            pltpu.VMEM((QUAD, K + 16, S), BF16),
            pltpu.VMEM((QUAD, 2 * K, K), F32),
            pltpu.VMEM((QUAD, 2 * K, K), BF16),
            pltpu.VMEM((QUAD, 2 * K, K), BF16),
            pltpu.VMEM((QUAD, K, K), BF16),
            pltpu.VMEM((QUAD, K, K), BF16),
            pltpu.VMEM((QUAD, K, K), BF16),
            pltpu.VMEM((QUAD, 1, S), F32),
            pltpu.SemaphoreType.DMA((4,)),
            pltpu.SemaphoreType.DMA((GROUPS,)),
            pltpu.SemaphoreType.DMA((GROUPS,)),
            pltpu.SemaphoreType.DMA((GROUPS, 2)),
            pltpu.SemaphoreType.DMA,
            pltpu.SemaphoreType.DMA,
            pltpu.SemaphoreType.DMA((GROUPS, 2)),
        ],
        compiler_params=pltpu.CompilerParams(
            collective_id=0, has_side_effects=True, vmem_limit_bytes=24 * 1024 * 1024
        ),
    )(*[pltpu.with_memory_space_constraint(arg, pltpu.HBM) for arg in (pairs, obs_site, obs_blocks, obs_precision, obs_innovation)])
    result = result.reshape(2, DEVICES, 4, PATCHES, 128).transpose(0, 1, 3, 2, 4)
    return result.reshape(2, DEVICES * PATCHES, S)


def solution(mesh):
    axes = ("member", "region")
    rows = P(axes, None)
    return jax.shard_map(
        local,
        mesh=mesh,
        in_specs=(P(axes, None, None), rows, P(axes), rows, rows),
        out_specs=P(axes, None, None),
        check_vma=False,
    )
```

```python
import functools

import jax
import jax.numpy as jnp
from jax import lax
from jax.experimental import pallas as pl
from jax.experimental.pallas import tpu as pltpu
from jax.sharding import PartitionSpec as P

K = 256
S = 512
SLOTS = 2048
OB = 128
ITERS = 6
EXACT_FROM = 4
DEVICES = 128
PATCHES = 8
GROUPS = 2
QUAD = PATCHES // GROUPS
STRIDE = 37
MESH = pl.DeviceIdType.MESH
F32 = jnp.float32
BF16 = jnp.bfloat16


def dot(left, right):
    return jnp.dot(left, right, preferred_element_type=F32)


def dot_t(left, right):
    return lax.dot_general(left, right, (((1,), (1,)), ((), ())), preferred_element_type=F32)


def split(value):
    high = value.astype(BF16)
    return high, (value - high.astype(F32)).astype(BF16)


def iota(shape, axis):
    return lax.broadcasted_iota(jnp.int32, shape, axis)


def hops(offset):
    return sum(min(step, 4 - step) for step in (offset % 4, offset // 4 % 4, offset // 16 % 4))


def spread(offset):
    return offset * STRIDE % DEVICES


OTHERS = sorted(range(1, DEVICES), key=spread)
FARTHEST_FIRST = sorted(OTHERS, key=lambda offset: (-hops(offset), spread(offset)))


def neighbours(member, region):
    xs = [lax.rem(lax.rem(region, 4) + step, 4) for step in range(4)]
    ys = [lax.rem(lax.div(region, 4) + step, 4) * 4 for step in range(4)]
    zs = [lax.rem(lax.div(member, 2) + step, 4) * 2 for step in range(4)]
    cores = [lax.rem(lax.rem(member, 2) + step, 2) for step in range(2)]

    def at(offset):
        return zs[offset // 16 % 4] + cores[offset // 64], ys[offset // 4 % 4] + xs[offset % 4]

    return at


def histogram(site_ref, blocks_ref, weight32, value32, tables):
    lanes = iota((1, SLOTS), 1)
    rows = iota((16, SLOTS), 0)
    quarter = lax.rem(rows, 4)

    def one(patch, carry):
        site = site_ref[pl.ds(patch, 1), :]
        live = lanes < blocks_ref[patch] * OB
        weight = jnp.where(live, weight32[pl.ds(patch, 1), :], 0.0)
        product = weight * value32[pl.ds(patch, 1), :]
        high = product.astype(BF16).astype(F32)
        low = product - high
        picked = jnp.where(rows < 4, weight, jnp.where(rows < 8, high, low))
        upper = jnp.where(quarter == lax.shift_right_logical(site, 7), picked, 0.0).astype(BF16)
        lower = jnp.where(iota((128, SLOTS), 0) == jnp.bitwise_and(site, 127), 1.0, 0.0).astype(BF16)
        sums = dot_t(upper, lower)
        tables[patch] = sums
        return carry

    lax.fori_loop(0, PATCHES, one, 0)


def as_row(table):
    return jnp.concatenate([table[part : part + 1, :] for part in range(4)], axis=1)


def analyse(group, inbox, outbox, place_in, place_out, tables, state, pert, work, iterate, high_part, low_part, product, product_low, coef, mean):
    landed = inbox.reshape(GROUPS + 1, 4, 4 * K, 128)
    leaving = outbox.reshape(GROUPS + 1, 4, 4 * K, 128)
    quads = range(QUAD)

    for block in range(4):
        rows = slice(256 * block, 256 * block + 256)
        for half in range(2):
            tile = jnp.concatenate([landed[group, 2 * half, rows, :], landed[group, 2 * half + 1, rows, :]], axis=1)
            placed = dot(place_in[...], tile).astype(BF16)
            for quad in quads:
                state[quad, 64 * block : 64 * block + 64, 256 * half : 256 * half + 256] = placed[
                    64 * quad : 64 * quad + 64
                ]

    eye = jnp.where(iota((K, K), 0) == iota((K, K), 1), 1.0, 0.0).astype(F32)
    scales, rights = [], []
    for quad in quads:
        table = tables[group * QUAD + quad]
        values = state[quad].astype(F32)
        centre = jnp.sum(values, axis=0, keepdims=True) * (1.0 / K)
        mean[quad] = jnp.broadcast_to(centre, (8, S))
        around = (values - centre).astype(BF16)
        pert[quad] = around
        work[quad, 0:K, :] = (around.astype(F32) * as_row(table[0:4])).astype(BF16)
        side = as_row(table[4:8] + table[8:12])
        high = side.astype(BF16).astype(F32)
        work[quad, K : K + 16, :] = jnp.where(
            iota((16, S), 0) == 0, high, jnp.where(iota((16, S), 0) == 1, side - high, 0.0)
        ).astype(BF16)
    for quad in quads:
        sums = dot_t(work[quad], pert[quad])
        right = sums[K : K + 1] + sums[K + 1 : K + 2]
        amat = sums[0:K] + 255.0 * eye
        square = jnp.sum(jnp.sum(amat * amat, axis=0, keepdims=True), axis=1, keepdims=True)
        scale = jnp.sqrt(square)
        scales.append(scale)
        rights.append(right)
        first = amat / scale
        iterate[quad, K:] = first
        high_part[quad, K:] = first.astype(BF16)
    for quad in quads:
        first = iterate[quad, K:]
        second = (eye - first * (1.0 / 3.0), first - dot(high_part[quad, K:], high_part[quad, K:]) * (1.0 / 3.0))
        for part in range(2):
            iterate[quad, K * part : K * part + K] = second[part]
            high_part[quad, K * part : K * part + K] = second[part].astype(BF16)

    for step in range(1, ITERS):
        exact = step >= EXACT_FROM
        last = step == ITERS - 1
        third = 1.5 ** (2 * step) / 3.0
        for quad in quads:
            z_high, y_high = high_part[quad, 0:K], high_part[quad, K:]
            both = dot(z_high, y_high)
            if exact:
                both += dot(z_high, low_part[quad, K:]) + dot(low_part[quad, 0:K], y_high)
                both = both * third
                product_low[quad] = (both - both.astype(BF16).astype(F32)).astype(BF16)
                product[quad] = both.astype(BF16)
            else:
                product[quad] = (both * third).astype(BF16)
        for quad in quads:
            for part in range(1 if last else 2):
                rows = slice(K * part, K * part + K)
                high = high_part[quad, rows]
                moved = dot(high, product[quad])
                if exact:
                    moved += dot(high, product_low[quad]) + dot(low_part[quad, rows], product[quad])
                after = iterate[quad, rows] - moved
                iterate[quad, rows] = after
                if not last:
                    high_part[quad, rows] = after.astype(BF16)
                    if step + 1 >= EXACT_FROM:
                        low_part[quad, rows] = (after - after.astype(BF16).astype(F32)).astype(BF16)

    grown = 1.5**ITERS
    for quad in quads:
        z = iterate[quad, 0:K]
        once = jnp.sum(z * rights[quad], axis=1, keepdims=True)
        twice = jnp.sum(z * once, axis=0, keepdims=True)
        factor = grown * jnp.sqrt(255.0 / scales[quad])
        coef[quad] = (twice * (grown * grown / scales[quad]) + factor * z).astype(BF16)
    for quad in quads:
        state[quad] = (mean[quad, 0:1] + dot(coef[quad], pert[quad])).astype(BF16)

    for block in range(4):
        rows = slice(256 * block, 256 * block + 256)
        for half in range(2):
            tile = jnp.concatenate(
                [state[quad, 64 * block : 64 * block + 64, 256 * half : 256 * half + 256] for quad in quads], axis=0
            )
            placed = dot(place_out[...], tile).astype(BF16)
            leaving[group, 2 * half, rows, :] = placed[:, 0:128]
            leaving[group, 2 * half + 1, rows, :] = placed[:, 128:256]


def kernel(
    ens_ref, site_hbm, blocks_hbm, precision_hbm, innovation_hbm, out_ref,
    site_ref, blocks_ref, precision_ref, innovation_ref, inbox, outbox, place_in, place_out, weight32, value32, tables, state, pert, work, iterate, high_part, low_part, product, product_low, coef, mean,
    obs_sem, in_send, in_recv, in_own, out_send, out_recv, out_own,
):
    member, region = lax.axis_index("member"), lax.axis_index("region")
    me = member * 16 + region

    moves = (
        pltpu.make_async_copy(site_hbm, site_ref, obs_sem.at[0]),
        pltpu.make_async_copy(precision_hbm, precision_ref, obs_sem.at[1]),
        pltpu.make_async_copy(innovation_hbm, innovation_ref, obs_sem.at[2]),
        pltpu.make_async_copy(blocks_hbm, blocks_ref, obs_sem.at[3]),
    )
    for move in moves:
        move.start()
    at = neighbours(member, region)

    def send_in(group, offsets):
        for offset in offsets:
            device = at(offset)
            for row in range(2):
                pltpu.make_async_remote_copy(
                    src_ref=ens_ref.at[row, device[0] * 16 + device[1], :, group],
                    dst_ref=inbox.at[group, :, me, row],
                    send_sem=in_send.at[group],
                    recv_sem=in_recv.at[group],
                    device_id=device,
                    device_id_type=MESH,
                ).start()

    barrier = pltpu.get_barrier_semaphore()
    for offset in FARTHEST_FIRST:
        pl.semaphore_signal(barrier, inc=1, device_id=at(offset), device_id_type=MESH)
    pl.semaphore_wait(barrier, DEVICES - 1)
    send_in(0, OTHERS)
    send_in(1, OTHERS)
    for group in range(GROUPS):
        for row in range(2):
            pltpu.make_async_copy(
                ens_ref.at[row, me, :, group], inbox.at[group, :, me, row], in_own.at[group, row]
            ).start()

    out_row, in_row = iota((256, 256), 0), iota((256, 256), 1)
    moved = jnp.bitwise_and(out_row, 63) * 4 + lax.shift_right_logical(out_row, 6)
    place_in[...] = jnp.where(in_row == moved, 1.0, 0.0).astype(BF16)
    moved = jnp.bitwise_and(out_row, 3) * 64 + lax.shift_right_logical(out_row, 2)
    place_out[...] = jnp.where(in_row == moved, 1.0, 0.0).astype(BF16)
    for move in moves:
        move.wait()
    weight32[...] = precision_ref[...].astype(F32)
    value32[...] = innovation_ref[...].astype(F32)
    histogram(site_ref, blocks_ref, weight32, value32, tables)

    def one_group(group, carry):
        for row in range(2):
            pltpu.make_async_copy(
                ens_ref.at[row, me, :, group], inbox.at[group, :, me, row], in_own.at[group, row]
            ).wait()
        arrived = inbox.at[group, :, pl.ds(0, DEVICES - 1)]
        pltpu.make_async_copy(arrived, arrived, in_recv.at[group]).wait()

        analyse(
            group, inbox, outbox, place_in, place_out, tables, state, pert, work, iterate, high_part, low_part, product, product_low, coef, mean
        )

        for offset in FARTHEST_FIRST:
            device = at(offset)
            for row in range(2):
                pltpu.make_async_remote_copy(
                    src_ref=outbox.at[group, :, device[0] * 16 + device[1], row],
                    dst_ref=out_ref.at[row, me, :, group],
                    send_sem=out_send,
                    recv_sem=out_recv,
                    device_id=device,
                    device_id_type=MESH,
                ).start()
        for row in range(2):
            pltpu.make_async_copy(
                outbox.at[group, :, me, row], out_ref.at[row, me, :, group], out_own.at[group, row]
            ).start()
        return carry

    lax.fori_loop(0, GROUPS, one_group, 0)

    for group in range(GROUPS):
        sent = inbox.at[group, :, pl.ds(0, DEVICES - 1)]
        pltpu.make_async_copy(sent, sent, in_send.at[group]).wait()
        for row in range(2):
            pltpu.make_async_copy(
                outbox.at[group, :, me, row], out_ref.at[row, me, :, group], out_own.at[group, row]
            ).wait()
    sent = outbox.at[pl.ds(0, GROUPS), :, pl.ds(0, DEVICES - 1)]
    pltpu.make_async_copy(sent, sent, out_send).wait()
    arrived = out_ref.at[:, pl.ds(0, DEVICES - 1)]
    pltpu.make_async_copy(arrived, arrived, out_recv).wait()


def local(ensemble, obs_site, obs_blocks, obs_precision, obs_innovation):
    pairs = ensemble.reshape(2, DEVICES, PATCHES, 4, 128).transpose(0, 1, 3, 2, 4)
    pairs = pairs.reshape(2, DEVICES, 4, GROUPS, QUAD, 128)
    hbm = pl.BlockSpec(memory_space=pltpu.HBM)
    result = pl.pallas_call(
        kernel,
        out_shape=jax.ShapeDtypeStruct(pairs.shape, BF16),
        in_specs=[hbm] * 5,
        out_specs=pl.BlockSpec(memory_space=pl.ANY),
        scratch_shapes=[
            pltpu.VMEM((PATCHES, SLOTS), jnp.int32),
            pltpu.SMEM((PATCHES,), jnp.int32),
            pltpu.VMEM((PATCHES, SLOTS), BF16),
            pltpu.VMEM((PATCHES, SLOTS), BF16),
            pltpu.VMEM((GROUPS + 1, 4, DEVICES, 2, QUAD, 128), BF16),
            pltpu.VMEM((GROUPS + 1, 4, DEVICES, 2, QUAD, 128), BF16),
            pltpu.VMEM((256, 256), BF16),
            pltpu.VMEM((256, 256), BF16),
            pltpu.VMEM((PATCHES, SLOTS), F32),
            pltpu.VMEM((PATCHES, SLOTS), F32),
            pltpu.VMEM((PATCHES, 16, 128), F32),
            pltpu.VMEM((QUAD, K, S), BF16),
            pltpu.VMEM((QUAD, K, S), BF16),
            pltpu.VMEM((QUAD, K + 16, S), BF16),
            pltpu.VMEM((QUAD, 2 * K, K), F32),
            pltpu.VMEM((QUAD, 2 * K, K), BF16),
            pltpu.VMEM((QUAD, 2 * K, K), BF16),
            pltpu.VMEM((QUAD, K, K), BF16),
            pltpu.VMEM((QUAD, K, K), BF16),
            pltpu.VMEM((QUAD, K, K), BF16),
            pltpu.VMEM((QUAD, 8, S), F32),
            pltpu.SemaphoreType.DMA((4,)),
            pltpu.SemaphoreType.DMA((GROUPS,)),
            pltpu.SemaphoreType.DMA((GROUPS,)),
            pltpu.SemaphoreType.DMA((GROUPS, 2)),
            pltpu.SemaphoreType.DMA,
            pltpu.SemaphoreType.DMA,
            pltpu.SemaphoreType.DMA((GROUPS, 2)),
        ],
        compiler_params=pltpu.CompilerParams(
            collective_id=0, has_side_effects=True, vmem_limit_bytes=24 * 1024 * 1024
        ),
    )(*[pltpu.with_memory_space_constraint(arg, pltpu.HBM) for arg in (pairs, obs_site, obs_blocks, obs_precision, obs_innovation)])
    result = result.reshape(2, DEVICES, 4, PATCHES, 128).transpose(0, 1, 3, 2, 4)
    return result.reshape(2, DEVICES * PATCHES, S)


def solution(mesh):
    axes = ("member", "region")
    rows = P(axes, None)
    return jax.shard_map(
        local,
        mesh=mesh,
        in_specs=(P(axes, None, None), rows, P(axes), rows, rows),
        out_specs=P(axes, None, None),
        check_vma=False,
    )
```

```python
import functools

import jax
import jax.numpy as jnp
from jax import lax
from jax.experimental import pallas as pl
from jax.experimental.pallas import tpu as pltpu
from jax.sharding import PartitionSpec as P

K = 256
S = 512
SLOTS = 2048
OB = 128
ITERS = 6
EXACT_FROM = 4
DEVICES = 128
PATCHES = 8
GROUPS = 2
QUAD = PATCHES // GROUPS
STRIDE = 37
MESH = pl.DeviceIdType.MESH
F32 = jnp.float32
BF16 = jnp.bfloat16


def dot(left, right):
    return jnp.dot(left, right, preferred_element_type=F32)


def dot_t(left, right):
    return lax.dot_general(left, right, (((1,), (1,)), ((), ())), preferred_element_type=F32)


def split(value):
    high = value.astype(BF16)
    return high, (value - high.astype(F32)).astype(BF16)


def iota(shape, axis):
    return lax.broadcasted_iota(jnp.int32, shape, axis)


def hops(offset):
    return sum(min(step, 4 - step) for step in (offset % 4, offset // 4 % 4, offset // 16 % 4))


def spread(offset):
    return offset * STRIDE % DEVICES


OTHERS = sorted(range(1, DEVICES), key=spread)
FARTHEST_FIRST = sorted(OTHERS, key=lambda offset: (-hops(offset), spread(offset)))
MIXED = [
    FARTHEST_FIRST[turn // 2 if turn % 2 == 0 else DEVICES - 2 - turn // 2] for turn in range(DEVICES - 1)
]


def neighbours(member, region):
    xs = [lax.rem(lax.rem(region, 4) + step, 4) for step in range(4)]
    ys = [lax.rem(lax.div(region, 4) + step, 4) * 4 for step in range(4)]
    zs = [lax.rem(lax.div(member, 2) + step, 4) * 2 for step in range(4)]
    cores = [lax.rem(lax.rem(member, 2) + step, 2) for step in range(2)]

    def at(offset):
        return zs[offset // 16 % 4] + cores[offset // 64], ys[offset // 4 % 4] + xs[offset % 4]

    return at


def histogram(site_ref, blocks_ref, weight32, value32, tables):
    lanes = iota((1, SLOTS), 1)
    rows = iota((16, SLOTS), 0)
    quarter = lax.rem(rows, 4)

    def one(patch, carry):
        site = site_ref[pl.ds(patch, 1), :]
        live = lanes < blocks_ref[patch] * OB
        weight = jnp.where(live, weight32[pl.ds(patch, 1), :], 0.0)
        product = weight * value32[pl.ds(patch, 1), :]
        high = product.astype(BF16).astype(F32)
        low = product - high
        picked = jnp.where(rows < 4, weight, jnp.where(rows < 8, high, low))
        upper = jnp.where(quarter == lax.shift_right_logical(site, 7), picked, 0.0).astype(BF16)
        lower = jnp.where(iota((128, SLOTS), 0) == jnp.bitwise_and(site, 127), 1.0, 0.0).astype(BF16)
        sums = dot_t(upper, lower)
        tables[patch] = sums
        return carry

    lax.fori_loop(0, PATCHES, one, 0)


def as_row(table):
    return jnp.concatenate([table[part : part + 1, :] for part in range(4)], axis=1)


def analyse(group, inbox, outbox, place_in, place_out, tables, state, pert, work, iterate, high_part, low_part, product, product_low, coef, mean):
    landed = inbox.reshape(GROUPS + 1, 4, 4 * K, 128)
    leaving = outbox.reshape(GROUPS + 1, 4, 4 * K, 128)
    quads = range(QUAD)

    for block in range(4):
        rows = slice(256 * block, 256 * block + 256)
        for half in range(2):
            tile = jnp.concatenate([landed[group, 2 * half, rows, :], landed[group, 2 * half + 1, rows, :]], axis=1)
            placed = dot(place_in[...], tile).astype(BF16)
            for quad in quads:
                state[quad, 64 * block : 64 * block + 64, 256 * half : 256 * half + 256] = placed[
                    64 * quad : 64 * quad + 64
                ]

    eye = jnp.where(iota((K, K), 0) == iota((K, K), 1), 1.0, 0.0).astype(F32)
    scales, rights = [], []
    for quad in quads:
        table = tables[group * QUAD + quad]
        values = state[quad].astype(F32)
        centre = jnp.sum(values, axis=0, keepdims=True) * (1.0 / K)
        mean[quad] = jnp.broadcast_to(centre, (8, S))
        around = (values - centre).astype(BF16)
        pert[quad] = around
        work[quad, 0:K, :] = (around.astype(F32) * as_row(table[0:4])).astype(BF16)
        side = as_row(table[4:8] + table[8:12])
        high = side.astype(BF16).astype(F32)
        work[quad, K : K + 16, :] = jnp.where(
            iota((16, S), 0) == 0, high, jnp.where(iota((16, S), 0) == 1, side - high, 0.0)
        ).astype(BF16)
    for quad in quads:
        sums = dot_t(work[quad], pert[quad])
        right = sums[K : K + 1] + sums[K + 1 : K + 2]
        amat = sums[0:K] + 255.0 * eye
        square = jnp.sum(jnp.sum(amat * amat, axis=0, keepdims=True), axis=1, keepdims=True)
        scale = jnp.sqrt(square)
        scales.append(scale)
        rights.append(right)
        first = amat / scale
        iterate[quad, K:] = first
        high_part[quad, K:] = first.astype(BF16)
    for quad in quads:
        first = iterate[quad, K:]
        second = (eye - first * (1.0 / 3.0), first - dot(high_part[quad, K:], high_part[quad, K:]) * (1.0 / 3.0))
        for part in range(2):
            iterate[quad, K * part : K * part + K] = second[part]
            high_part[quad, K * part : K * part + K] = second[part].astype(BF16)

    for step in range(1, ITERS):
        exact = step >= EXACT_FROM
        last = step == ITERS - 1
        third = 1.5 ** (2 * step) / 3.0
        for quad in quads:
            z_high, y_high = high_part[quad, 0:K], high_part[quad, K:]
            both = dot(z_high, y_high)
            if exact:
                both += dot(z_high, low_part[quad, K:]) + dot(low_part[quad, 0:K], y_high)
                both = both * third
                product_low[quad] = (both - both.astype(BF16).astype(F32)).astype(BF16)
                product[quad] = both.astype(BF16)
            else:
                product[quad] = (both * third).astype(BF16)
        for quad in quads:
            for part in range(1 if last else 2):
                rows = slice(K * part, K * part + K)
                high = high_part[quad, rows]
                moved = dot(high, product[quad])
                if exact:
                    moved += dot(high, product_low[quad]) + dot(low_part[quad, rows], product[quad])
                after = iterate[quad, rows] - moved
                iterate[quad, rows] = after
                if not last:
                    high_part[quad, rows] = after.astype(BF16)
                    if step + 1 >= EXACT_FROM:
                        low_part[quad, rows] = (after - after.astype(BF16).astype(F32)).astype(BF16)

    grown = 1.5**ITERS
    for quad in quads:
        z = iterate[quad, 0:K]
        once = jnp.sum(z * rights[quad], axis=1, keepdims=True)
        twice = jnp.sum(z * once, axis=0, keepdims=True)
        factor = grown * jnp.sqrt(255.0 / scales[quad])
        coef[quad] = (twice * (grown * grown / scales[quad]) + factor * z).astype(BF16)
    for quad in quads:
        state[quad] = (mean[quad, 0:1] + dot(coef[quad], pert[quad])).astype(BF16)

    for block in range(4):
        rows = slice(256 * block, 256 * block + 256)
        for half in range(2):
            tile = jnp.concatenate(
                [state[quad, 64 * block : 64 * block + 64, 256 * half : 256 * half + 256] for quad in quads], axis=0
            )
            placed = dot(place_out[...], tile).astype(BF16)
            leaving[group, 2 * half, rows, :] = placed[:, 0:128]
            leaving[group, 2 * half + 1, rows, :] = placed[:, 128:256]


def kernel(
    ens_ref, site_hbm, blocks_hbm, precision_hbm, innovation_hbm, out_ref,
    site_ref, blocks_ref, precision_ref, innovation_ref, inbox, outbox, place_in, place_out, weight32, value32, tables, state, pert, work, iterate, high_part, low_part, product, product_low, coef, mean,
    obs_sem, in_send, in_recv, in_own, out_send, out_recv, out_own,
):
    member, region = lax.axis_index("member"), lax.axis_index("region")
    me = member * 16 + region

    moves = (
        pltpu.make_async_copy(site_hbm, site_ref, obs_sem.at[0]),
        pltpu.make_async_copy(precision_hbm, precision_ref, obs_sem.at[1]),
        pltpu.make_async_copy(innovation_hbm, innovation_ref, obs_sem.at[2]),
        pltpu.make_async_copy(blocks_hbm, blocks_ref, obs_sem.at[3]),
    )
    for move in moves:
        move.start()
    at = neighbours(member, region)

    def send_in(group, offsets):
        for offset in offsets:
            device = at(offset)
            for row in range(2):
                pltpu.make_async_remote_copy(
                    src_ref=ens_ref.at[row, device[0] * 16 + device[1], :, group],
                    dst_ref=inbox.at[group, :, me, row],
                    send_sem=in_send.at[group],
                    recv_sem=in_recv.at[group],
                    device_id=device,
                    device_id_type=MESH,
                ).start()

    barrier = pltpu.get_barrier_semaphore()
    for offset in FARTHEST_FIRST:
        pl.semaphore_signal(barrier, inc=1, device_id=at(offset), device_id_type=MESH)
    pl.semaphore_wait(barrier, DEVICES - 1)
    send_in(0, MIXED)
    send_in(1, MIXED)
    for group in range(GROUPS):
        for row in range(2):
            pltpu.make_async_copy(
                ens_ref.at[row, me, :, group], inbox.at[group, :, me, row], in_own.at[group, row]
            ).start()

    out_row, in_row = iota((256, 256), 0), iota((256, 256), 1)
    moved = jnp.bitwise_and(out_row, 63) * 4 + lax.shift_right_logical(out_row, 6)
    place_in[...] = jnp.where(in_row == moved, 1.0, 0.0).astype(BF16)
    moved = jnp.bitwise_and(out_row, 3) * 64 + lax.shift_right_logical(out_row, 2)
    place_out[...] = jnp.where(in_row == moved, 1.0, 0.0).astype(BF16)
    for move in moves:
        move.wait()
    weight32[...] = precision_ref[...].astype(F32)
    value32[...] = innovation_ref[...].astype(F32)
    histogram(site_ref, blocks_ref, weight32, value32, tables)

    def one_group(group, carry):
        for row in range(2):
            pltpu.make_async_copy(
                ens_ref.at[row, me, :, group], inbox.at[group, :, me, row], in_own.at[group, row]
            ).wait()
        arrived = inbox.at[group, :, pl.ds(0, DEVICES - 1)]
        pltpu.make_async_copy(arrived, arrived, in_recv.at[group]).wait()

        analyse(
            group, inbox, outbox, place_in, place_out, tables, state, pert, work, iterate, high_part, low_part, product, product_low, coef, mean
        )

        for offset in FARTHEST_FIRST:
            device = at(offset)
            for row in range(2):
                pltpu.make_async_remote_copy(
                    src_ref=outbox.at[group, :, device[0] * 16 + device[1], row],
                    dst_ref=out_ref.at[row, me, :, group],
                    send_sem=out_send,
                    recv_sem=out_recv,
                    device_id=device,
                    device_id_type=MESH,
                ).start()
        for row in range(2):
            pltpu.make_async_copy(
                outbox.at[group, :, me, row], out_ref.at[row, me, :, group], out_own.at[group, row]
            ).start()
        return carry

    lax.fori_loop(0, GROUPS, one_group, 0)

    for group in range(GROUPS):
        sent = inbox.at[group, :, pl.ds(0, DEVICES - 1)]
        pltpu.make_async_copy(sent, sent, in_send.at[group]).wait()
        for row in range(2):
            pltpu.make_async_copy(
                outbox.at[group, :, me, row], out_ref.at[row, me, :, group], out_own.at[group, row]
            ).wait()
    sent = outbox.at[pl.ds(0, GROUPS), :, pl.ds(0, DEVICES - 1)]
    pltpu.make_async_copy(sent, sent, out_send).wait()
    arrived = out_ref.at[:, pl.ds(0, DEVICES - 1)]
    pltpu.make_async_copy(arrived, arrived, out_recv).wait()


def local(ensemble, obs_site, obs_blocks, obs_precision, obs_innovation):
    pairs = ensemble.reshape(2, DEVICES, PATCHES, 4, 128).transpose(0, 1, 3, 2, 4)
    pairs = pairs.reshape(2, DEVICES, 4, GROUPS, QUAD, 128)
    hbm = pl.BlockSpec(memory_space=pltpu.HBM)
    result = pl.pallas_call(
        kernel,
        out_shape=jax.ShapeDtypeStruct(pairs.shape, BF16),
        in_specs=[hbm] * 5,
        out_specs=pl.BlockSpec(memory_space=pl.ANY),
        scratch_shapes=[
            pltpu.VMEM((PATCHES, SLOTS), jnp.int32),
            pltpu.SMEM((PATCHES,), jnp.int32),
            pltpu.VMEM((PATCHES, SLOTS), BF16),
            pltpu.VMEM((PATCHES, SLOTS), BF16),
            pltpu.VMEM((GROUPS + 1, 4, DEVICES, 2, QUAD, 128), BF16),
            pltpu.VMEM((GROUPS + 1, 4, DEVICES, 2, QUAD, 128), BF16),
            pltpu.VMEM((256, 256), BF16),
            pltpu.VMEM((256, 256), BF16),
            pltpu.VMEM((PATCHES, SLOTS), F32),
            pltpu.VMEM((PATCHES, SLOTS), F32),
            pltpu.VMEM((PATCHES, 16, 128), F32),
            pltpu.VMEM((QUAD, K, S), BF16),
            pltpu.VMEM((QUAD, K, S), BF16),
            pltpu.VMEM((QUAD, K + 16, S), BF16),
            pltpu.VMEM((QUAD, 2 * K, K), F32),
            pltpu.VMEM((QUAD, 2 * K, K), BF16),
            pltpu.VMEM((QUAD, 2 * K, K), BF16),
            pltpu.VMEM((QUAD, K, K), BF16),
            pltpu.VMEM((QUAD, K, K), BF16),
            pltpu.VMEM((QUAD, K, K), BF16),
            pltpu.VMEM((QUAD, 8, S), F32),
            pltpu.SemaphoreType.DMA((4,)),
            pltpu.SemaphoreType.DMA((GROUPS,)),
            pltpu.SemaphoreType.DMA((GROUPS,)),
            pltpu.SemaphoreType.DMA((GROUPS, 2)),
            pltpu.SemaphoreType.DMA,
            pltpu.SemaphoreType.DMA,
            pltpu.SemaphoreType.DMA((GROUPS, 2)),
        ],
        compiler_params=pltpu.CompilerParams(
            collective_id=0, has_side_effects=True, vmem_limit_bytes=24 * 1024 * 1024
        ),
    )(*[pltpu.with_memory_space_constraint(arg, pltpu.HBM) for arg in (pairs, obs_site, obs_blocks, obs_precision, obs_innovation)])
    result = result.reshape(2, DEVICES, 4, PATCHES, 128).transpose(0, 1, 3, 2, 4)
    return result.reshape(2, DEVICES * PATCHES, S)


def solution(mesh):
    axes = ("member", "region")
    rows = P(axes, None)
    return jax.shard_map(
        local,
        mesh=mesh,
        in_specs=(P(axes, None, None), rows, P(axes), rows, rows),
        out_specs=P(axes, None, None),
        check_vma=False,
    )
```
